32 devices in a mesh: row: 8 (over z, y), col: 4 (over x, core).
Axes of the slice: x: 2, y: 2, z: 4, core: 2. Of those that a mesh axis runs over, the one named last changes fastest.
Arguments:
- spectra: bfloat16 [1024, 16, 128], P(('row', 'col')), may hold values from -4 to 4
- window_flags: int32 [1024, 64], P(('row', 'col')), may hold values 0 or 1
- pair_mask: int32 [1024, 1024], P('row', 'col'), may hold values 0 or 1
- misfit_weight: bfloat16 [16, 1024, 1024], P(None, 'row', 'col'), may hold values from 0.0099487305 to 0.099609375
- observed: bfloat16 [2, 16, 1024, 1024], P(None, None, 'row', 'col'), may hold values from -6 to 6
Outputs:
- grad_first: bfloat16 [1024, 16, 128], P(('row', 'col'))
- grad_second: bfloat16 [4, 256, 16, 128], P('col', 'row')
The draws below stay inside these ranges and needn't reach their ends.
All inputs are finite; a program needn't handle non-finite values. No bound on the sum of `window_flags` or of `pair_mask` on one device may be relied on, other than what follows from the above.
Results may differ from the reference program's by a relative error of at most 0.019.
Values may be sent and summed in bfloat16 or wider, within the bound.
No kernel may reach another device: no remote copies, remote signals or barrier semaphores. Data moves between devices by JAX's collectives and lax.ppermute only.
A program may use at most 64 MiB of HBM per device.

```python
import math
import jax
import jax.numpy as jnp
from jax import lax

ROW_BLOCK = 128
FREQS = 16
WINDOWS = 64
STATIONS = 1024
N_ROW = 8
N_COL = 4


def with_ends(values, stream_key, smallest, largest):
    longest = values.shape.index(max(values.shape))
    spots = []
    for shift in (0, 1):
        where = [jax.random.randint(jax.random.fold_in(stream_key, axis), (), 0, length) for axis, length in enumerate(values.shape)]
        where[longest] = (where[longest] + shift) % values.shape[longest]
        spots.append(tuple(where))
    return values.at[spots[0]].set(smallest).at[spots[1]].set(largest)


def levels(stream_key, shape, split, low, high):
    def one(axis_at, parts):
        heights = jax.random.uniform(jax.random.fold_in(jax.random.fold_in(stream_key, 6), axis_at), (parts,), jnp.float32, low / len(split), high / len(split))
        return jnp.repeat(jnp.exp(heights), shape[axis_at] // parts).reshape((-1,) + (1,) * (len(shape) - axis_at - 1))

    gain = one(*split[0])
    for cut in split[1:]:
        gain = gain * one(*cut)
    return gain


def noise(own_key, dims, deviation, bound, pieces=(), held_as=jnp.bfloat16):
    array = jax.random.normal(own_key, dims, jnp.float32) * deviation
    if len(pieces) > 0:
        array = levels(own_key, dims, pieces, -0.22, 0.18) * array
    return jnp.clip(array, min=-bound, max=bound).astype(held_as)


def setup_inputs(seed: int = 0) -> dict:
    seeds = jax.random.split(jax.random.key(seed), 6)
    spectra = noise(seeds[0], (STATIONS, FREQS, 2 * WINDOWS), 0.3, 4.0, ((0, 32),))
    window_flags = with_ends((jax.random.randint(seeds[1], (STATIONS, WINDOWS), 0, 4) < 3).astype(jnp.int32), jax.random.fold_in(seeds[1], 1), 0, 1)
    pair_mask = with_ends((jax.random.randint(seeds[2], (STATIONS, STATIONS), 0, 5) < 3).astype(jnp.int32), jax.random.fold_in(seeds[2], 1), 0, 1)
    misfit_weight = jnp.clip(jnp.exp(math.log(0.099609375) - 2.3038113 * jax.random.uniform(seeds[3], (FREQS, STATIONS, STATIONS), jnp.float32) ** levels(seeds[3], (FREQS, STATIONS, STATIONS), ((1, 8), (2, 4)), -0.2, 0.2)), 0.0099487305, 0.099609375).astype(jnp.bfloat16)
    observed = noise(seeds[4], (2, FREQS, STATIONS, STATIONS), 1.0, 6.0, ((2, 8), (3, 4)))
    return dict(spectra=spectra, window_flags=window_flags, pair_mask=pair_mask, misfit_weight=misfit_weight, observed=observed)


def reference(spectra, window_flags, pair_mask, misfit_weight, observed):
    half_width = spectra.shape[2] // 2
    flag_value = window_flags.astype(jnp.float32)
    flag_both = jnp.concatenate([flag_value, flag_value], axis=1)
    flagged = (spectra.astype(jnp.float32) * flag_both[:, None, :]).astype(jnp.bfloat16)
    flagged_wide = flagged.astype(jnp.float32)
    swapped = jnp.concatenate([-flagged_wide[..., half_width:], flagged_wide[..., :half_width]], axis=-1)
    col_stack = jnp.stack([flagged_wide, swapped])
    row_stack = jnp.stack([flagged_wide, -swapped])
    col_block = STATIONS // N_COL
    mask_wide = pair_mask.astype(jnp.float32)
    weight_wide = misfit_weight.astype(jnp.float32)
    observed_wide = observed.astype(jnp.float32)
    split_col = col_stack.reshape(2, N_COL, col_block, FREQS, 2 * WINDOWS)

    def one_block(accum_second, block_index):
        first_row = (block_index * ROW_BLOCK).astype(jnp.int32)
        row_part = lax.dynamic_slice_in_dim(flagged_wide, first_row, ROW_BLOCK, 0)
        row_pair = lax.dynamic_slice_in_dim(row_stack, first_row, ROW_BLOCK, 1)
        mask_part = lax.dynamic_slice_in_dim(mask_wide, first_row, ROW_BLOCK, 0)
        weight_part = lax.dynamic_slice_in_dim(weight_wide, first_row, ROW_BLOCK, 1)
        observed_part = lax.dynamic_slice_in_dim(observed_wide, first_row, ROW_BLOCK, 2)
        cross_spec = jnp.einsum('ifk,cjfk->cfij', row_part, col_stack, precision=lax.Precision.HIGHEST)
        residual = (mask_part[None, None] * weight_part[None] * (cross_spec - observed_part)).astype(jnp.bfloat16)
        residual = lax.optimization_barrier(residual).astype(jnp.float32)
        split_res = residual.reshape(2, FREQS, ROW_BLOCK, N_COL, col_block)
        first_terms = jnp.einsum('cfinj,cnjfk->nifk', split_res, split_col, precision=lax.Precision.HIGHEST)
        first_terms = lax.optimization_barrier(first_terms.astype(jnp.bfloat16)).astype(jnp.float32)
        first_grad = jnp.sum(first_terms, axis=0).astype(jnp.bfloat16)
        second_terms = jnp.einsum('cfij,cifk->jfk', residual, row_pair, precision=lax.Precision.HIGHEST)
        second_terms = lax.optimization_barrier(second_terms.astype(jnp.bfloat16)).astype(jnp.float32)
        return accum_second + second_terms, first_grad

    initial = jnp.zeros((STATIONS, FREQS, 2 * WINDOWS), jnp.float32)
    accum_second, firsts = lax.scan(one_block, initial, jnp.arange(N_ROW, dtype=jnp.int32))
    grad_first = firsts.reshape(STATIONS, FREQS, 2 * WINDOWS)
    grad_second = accum_second.astype(jnp.bfloat16).reshape(N_COL, col_block, FREQS, 2 * WINDOWS)
    return grad_first, grad_second
```

```python
import functools

import jax
import jax.numpy as jnp
from jax import lax
from jax.experimental import pallas as pl
from jax.experimental.pallas import tpu as pltpu
from jax.sharding import PartitionSpec as P


AXES = ("row", "col")
F32 = jnp.float32
BF16 = jnp.bfloat16


def chunk_sizes(freqs):
    half = freqs // 2
    return (half, freqs - half)


def vmem(count):
    return [pl.BlockSpec(memory_space=pltpu.VMEM)] * count


def grid_place(cols, ratio):
    row = lax.axis_index("row")
    return row // ratio, row % ratio, lax.axis_index("col")


def kernel_call(body, name, outs, scratch, flops, args):
    moved = sum(a.size * a.dtype.itemsize for a in args)
    return pl.pallas_call(
        body,
        name=name,
        out_shape=[jax.ShapeDtypeStruct(*o) for o in outs],
        in_specs=vmem(len(args)),
        out_specs=vmem(len(outs)),
        scratch_shapes=scratch,
        cost_estimate=pl.CostEstimate(
            flops=flops, bytes_accessed=moved, transcendentals=0
        ),
    )(*args)


def flag_body(sizes, spectra, flags, *refs):
    outs, wide = refs[:-1], refs[-1]
    n, freqs, width = spectra.shape
    half = flags.shape[1]
    spread = lax.broadcasted_iota(jnp.int32, (half, width), 1) % half
    spread = (spread == lax.broadcasted_iota(jnp.int32, (half, width), 0)).astype(BF16)
    both = jnp.dot(flags[...].astype(F32).astype(BF16), spread, preferred_element_type=F32)
    wide[...] = spectra[...].astype(F32).reshape(n * freqs, width)
    f = 0
    for size, out in zip(sizes, outs):
        for i in range(size):
            out[i] = (wide[pl.ds(f, n, stride=freqs), :] * both).astype(BF16)
            f += 1


def join_body(cols, ratio, *refs):
    pieces, out = refs[:-1], refs[-1]
    plane, _, _ = grid_place(cols, ratio)
    n = pieces[0].shape[1]
    for k, piece in enumerate(pieces):
        slot = lax.rem(plane + cols - k, cols)
        out[:, pl.ds(pl.multiple_of(slot * n, n), n), :] = piece[...]


def pair_body(cols, ratio, start, *refs):
    first, rest = refs[:cols], refs[cols:]
    second, rest = rest[:ratio], rest[ratio:]
    mask, weight, observed = rest[:3]
    rest = rest[3:]
    first_out, rest = rest[:cols], rest[cols:]
    second_out, rest = rest[:ratio], rest[ratio:]
    left, right, first_sum, second_sum = rest
    _, turn, col = grid_place(cols, ratio)
    size, n, width = first[0].shape
    rows = cols * n
    for k in range(cols):
        slot = lax.rem(col + cols - k, cols)
        left[:, pl.ds(pl.multiple_of(slot * n, n), n), :] = first[k][...]
    for k in range(ratio):
        slot = lax.rem(turn + ratio - k, ratio)
        right[:, pl.ds(pl.multiple_of(slot * rows, rows), rows), :] = second[k][...]
    valid = mask[...].astype(F32)
    lane = lax.broadcasted_iota(jnp.int32, (rows, width), 1)
    sign = jnp.where(lane < width // 2, 1.0, -1.0).astype(F32)

    def one(i, _):
        mine = left[i]
        turned = (pltpu.roll(mine.astype(F32), width // 2, 1) * sign).astype(BF16)
        stack = jnp.concatenate([mine, turned], axis=0)
        other = right[i]
        cross = lax.dot_general(
            stack, other, (((1,), (1,)), ((), ())), preferred_element_type=F32
        )
        scale = valid * weight[start + i].astype(F32)
        real = scale * (cross[:rows] - observed[0, start + i].astype(F32))
        imag = scale * (cross[rows:] - observed[1, start + i].astype(F32))
        residual = jnp.concatenate([real.astype(BF16), imag.astype(BF16)], axis=0)
        both = jnp.dot(residual, other, preferred_element_type=F32)
        grad = both[:rows] - pltpu.roll(both[rows:], width // 2, 1) * sign
        first_sum[i] = grad.astype(BF16)
        second_sum[i] = lax.dot_general(
            residual, stack, (((0,), (0,)), ((), ())), preferred_element_type=F32
        ).astype(BF16)
        return 0

    lax.fori_loop(0, size, one, 0, unroll=2)
    for k in range(cols):
        slot = lax.rem(col + k, cols)
        first_out[k][...] = first_sum[:, pl.ds(pl.multiple_of(slot * n, n), n), :]
    for k in range(ratio):
        slot = lax.rem(turn + k, ratio)
        for p in range(cols):
            at = pl.multiple_of((p * ratio + slot) * n, n)
            second_out[k][:, p * n : (p + 1) * n, :] = second_sum[:, pl.ds(at, n), :]


def fold_body(cols, ratio, *refs):
    terms, outs = refs[:ratio], refs[ratio:]
    plane, _, _ = grid_place(cols, ratio)
    n = outs[0].shape[1]
    for k, out in enumerate(outs):
        slot = lax.rem(plane + k, cols)
        where = pl.ds(pl.multiple_of(slot * n, n), n)
        total = terms[0][:, where, :].astype(F32)
        for term in terms[1:]:
            total += term[:, where, :].astype(F32)
        out[...] = total.astype(BF16)


def finish_body(sizes, cols, *refs):
    out, wide = refs[-2:]
    n, freqs, width = out.shape
    f = 0
    for q, size in enumerate(sizes):
        terms = refs[q * cols : (q + 1) * cols]
        for i in range(size):
            total = terms[0][i].astype(F32)
            for term in terms[1:]:
                total += term[i].astype(F32)
            wide[pl.ds(f, n, stride=freqs), :] = total
            f += 1
    out[...] = wide[...].reshape(n, freqs, width).astype(BF16)


def per_device(row_count, col_count, spectra, window_flags, pair_mask, misfit_weight, observed):
    ratio = row_count // col_count
    n, freqs, width = spectra.shape
    sizes = chunk_sizes(freqs)
    rows, others = col_count * n, row_count * n

    def route(where):
        pairs = []
        for row in range(row_count):
            for col in range(col_count):
                plane, turn, to = where(row // ratio, row % ratio, col)
                pairs.append((row * col_count + col, (plane * ratio + turn) * col_count + to))
        return pairs

    to_second = [
        route(lambda z, t, c, k=k: ((c + k) % col_count, t, z)) for k in range(col_count)
    ]
    along_col = [
        route(lambda z, t, c, k=k: (z, t, (c + k) % col_count)) for k in range(col_count)
    ]
    along_turn = [route(lambda z, t, c, k=k: (z, (t + k) % ratio, c)) for k in range(ratio)]
    along_plane = [
        route(lambda z, t, c, k=k: ((z + k) % col_count, t, c)) for k in range(col_count)
    ]

    def send(value, pairs):
        return lax.ppermute(value, AXES, pairs)

    def spread_over(values, routes):
        return [values[0]] + [send(v, p) for v, p in zip(values[1:], routes[1:])]

    flagged = kernel_call(
        functools.partial(flag_body, sizes),
        "flag",
        [((size, n, width), BF16) for size in sizes],
        [pltpu.VMEM((n * freqs, width), F32)],
        2 * spectra.size,
        (spectra, window_flags),
    )
    first_terms, second_terms = [], []
    start = 0
    for size, own in zip(sizes, flagged):
        pieces = [send(own, p) for p in to_second]
        first = spread_over([own] * col_count, along_col)
        (block,) = kernel_call(
            functools.partial(join_body, col_count, ratio),
            "join",
            [((size, rows, width), BF16)],
            [],
            own.size,
            pieces,
        )
        second = spread_over([block] * ratio, along_turn)
        outs = kernel_call(
            functools.partial(pair_body, col_count, ratio, start),
            "pair",
            [((size, n, width), BF16)] * col_count + [((size, rows, width), BF16)] * ratio,
            [
                pltpu.VMEM((size, rows, width), BF16),
                pltpu.VMEM((size, others, width), BF16),
                pltpu.VMEM((size, rows, width), BF16),
                pltpu.VMEM((size, others, width), BF16),
            ],
            12 * size * rows * others * width,
            (*first, *second, pair_mask, misfit_weight, observed),
        )
        halves = spread_over(outs[col_count:], along_turn)
        first_terms += spread_over(outs[:col_count], along_col)
        quarters = kernel_call(
            functools.partial(fold_body, col_count, ratio),
            "fold",
            [((size, n, width), BF16)] * col_count,
            [],
            ratio * halves[0].size,
            halves,
        )
        second_terms += spread_over(quarters, along_plane)
        start += size

    def finish(terms, name):
        (out,) = kernel_call(
            functools.partial(finish_body, sizes, col_count),
            name,
            [((n, freqs, width), BF16)],
            [pltpu.VMEM((n * freqs, width), F32)],
            col_count * spectra.size,
            terms,
        )
        return out

    grad_first = finish(first_terms, "finish_first")
    grad_second = finish(second_terms, "finish_second")
    return grad_first, grad_second[None]


def solution(mesh):
    placed = (
        P(AXES, None, None),
        P(AXES, None),
        P("row", "col"),
        P(None, "row", "col"),
        P(None, None, "row", "col"),
    )
    return jax.shard_map(
        functools.partial(per_device, mesh.shape["row"], mesh.shape["col"]),
        mesh=mesh,
        in_specs=placed,
        out_specs=(P(AXES, None, None), P("col", "row", None, None)),
        check_vma=False,
    )
```

```python
import functools
import math

import jax
import jax.numpy as jnp
from jax import lax
from jax.experimental import pallas as pl
from jax.experimental.pallas import tpu as pltpu
from jax.sharding import PartitionSpec as P


AXES = ("row", "col")
F32 = jnp.float32
BF16 = jnp.bfloat16
SPARE = 2 << 20
PARTS = 2
WAIT_FLOPS = 5 * 10**9


def chunk_sizes(freqs):
    bounds = [freqs * q // PARTS for q in range(PARTS + 1)]
    return tuple(b - a for a, b in zip(bounds, bounds[1:]))


def grid_place(ratio):
    row = lax.axis_index("row")
    return row // ratio, row % ratio, lax.axis_index("col")


def kernel_call(body, outs, scratch, flops, args):
    shapes = [jax.ShapeDtypeStruct(*o) for o in outs]
    moved = sum(a.size * a.dtype.itemsize for a in (*args, *shapes))
    held = sum(math.prod(m.shape) * jnp.dtype(m.dtype).itemsize for m in scratch)
    near = pl.BlockSpec(memory_space=pltpu.VMEM)
    return pl.pallas_call(
        body,
        out_shape=shapes,
        in_specs=[near] * len(args),
        out_specs=[near] * len(outs),
        scratch_shapes=scratch,
        compiler_params=pltpu.CompilerParams(vmem_limit_bytes=moved + held + SPARE),
        cost_estimate=pl.CostEstimate(
            flops=flops, bytes_accessed=moved, transcendentals=0
        ),
    )(*args)


def flag_body(sizes, spectra, flags, *refs):
    whole, outs, wide = refs[0], refs[1:-1], refs[-1]
    n, freqs, width = spectra.shape
    half = flags.shape[1]
    spread = lax.broadcasted_iota(jnp.int32, (half, width), 1) % half
    spread = (spread == lax.broadcasted_iota(jnp.int32, (half, width), 0)).astype(BF16)
    both = jnp.dot(flags[...].astype(F32).astype(BF16), spread, preferred_element_type=F32)
    wide[...] = spectra[...].astype(F32).reshape(n * freqs, width)
    f = 0
    for size, out in zip(sizes, outs):
        for i in range(size):
            out[i] = whole[f] = (wide[pl.ds(f, n, stride=freqs), :] * both).astype(BF16)
            f += 1


def join_body(cols, ratio, *refs):
    pieces, out = refs[:-1], refs[-1]
    plane, _, _ = grid_place(ratio)
    n = pieces[0].shape[1]
    for k, piece in enumerate(pieces):
        slot = lax.rem(plane + cols - k, cols)
        out[:, pl.ds(pl.multiple_of(slot * n, n), n), :] = piece[...]


def pair_body(cols, ratio, start, done, *refs):
    first, rest = refs[:cols], refs[cols:]
    second, rest = rest[:ratio], rest[ratio:]
    earlier, rest = rest[:done], rest[done:]
    mask, weight, observed = rest[:3]
    second_out, rest = rest[3 : 3 + ratio], rest[3 + ratio :]
    first_out, scratch = rest[:-4], rest[-4:]
    left, right, first_sum, second_sum = scratch
    _, turn, col = grid_place(ratio)
    size, rows, width = left.shape
    n = rows // cols

    chunk = pl.ds(start, size)
    for k in range(cols):
        slot = lax.rem(col + cols - k, cols)
        left[:, pl.ds(pl.multiple_of(slot * n, n), n), :] = first[k][chunk]
    for k in range(ratio):
        slot = lax.rem(turn + ratio - k, ratio)
        right[:, pl.ds(pl.multiple_of(slot * rows, rows), rows), :] = second[k][...]
    valid = mask[...].astype(F32)
    lane = lax.broadcasted_iota(jnp.int32, (rows, width), 1)
    sign = jnp.where(lane < width // 2, 1.0, -1.0).astype(F32)

    def one(i, _):
        mine = left[i]
        turned = (pltpu.roll(mine.astype(F32), width // 2, 1) * sign).astype(BF16)
        stack = jnp.concatenate([mine, turned], axis=0)
        other = right[i]
        cross = lax.dot_general(
            stack, other, (((1,), (1,)), ((), ())), preferred_element_type=F32
        )
        scale = valid * weight[start + i].astype(F32)
        real = scale * (cross[:rows] - observed[0, start + i].astype(F32))
        imag = scale * (cross[rows:] - observed[1, start + i].astype(F32))
        residual = jnp.concatenate([real.astype(BF16), imag.astype(BF16)], axis=0)
        both = jnp.dot(residual, other, preferred_element_type=F32)
        grad = both[:rows] - pltpu.roll(both[rows:], width // 2, 1) * sign
        first_sum[i] = grad.astype(BF16)
        second_sum[i] = lax.dot_general(
            residual, stack, (((0,), (0,)), ((), ())), preferred_element_type=F32
        ).astype(BF16)
        return 0

    lax.fori_loop(0, size, one, 0, unroll=2)
    for k in range(ratio):
        slot = lax.rem(turn + k, ratio)
        for p in range(cols):
            at = pl.multiple_of((p * ratio + slot) * n, n)
            second_out[k][:, p * n : (p + 1) * n, :] = second_sum[:, pl.ds(at, n), :]
    if len(first_out) == 1:
        first_out[0][...] = first_sum[...]
        return
    for k, out in enumerate(first_out):
        slot = lax.rem(col + k, cols)
        where = pl.ds(pl.multiple_of(slot * n, n), n)
        f = 0
        for part in (*earlier, first_sum):
            out[f : f + part.shape[0]] = part[:, where, :]
            f += part.shape[0]


def fold_body(cols, ratio, *refs):
    terms, outs = refs[:ratio], refs[ratio:]
    plane, _, _ = grid_place(ratio)
    n = outs[0].shape[1]
    for k, out in enumerate(outs):
        slot = lax.rem(plane + k, cols)
        where = pl.ds(pl.multiple_of(slot * n, n), n)
        total = terms[0][:, where, :].astype(F32)
        for term in terms[1:]:
            total += term[:, where, :].astype(F32)
        out[...] = total.astype(BF16)


def finish_body(sizes, *refs):
    out, wide = refs[-2:]
    n, freqs, width = out.shape
    count = (len(refs) - 2) // len(sizes)
    f = 0
    for q, size in enumerate(sizes):
        terms = refs[q * count : (q + 1) * count]
        for i in range(size):
            total = terms[0][i].astype(F32)
            for term in terms[1:]:
                total += term[i].astype(F32)
            wide[pl.ds(f, n, stride=freqs), :] = total
            f += 1
    out[...] = wide[...].reshape(n, freqs, width).astype(BF16)


def per_device(row_count, col_count, spectra, window_flags, pair_mask, misfit_weight, observed):
    ratio = row_count // col_count
    n, freqs, width = spectra.shape
    sizes = chunk_sizes(freqs)
    rows, others = col_count * n, row_count * n

    def route(where):
        pairs = []
        for row in range(row_count):
            for col in range(col_count):
                plane, turn, to = where(row // ratio, row % ratio, col)
                pairs.append((row * col_count + col, (plane * ratio + turn) * col_count + to))
        return pairs

    to_second = [
        route(lambda z, t, c, k=k: ((c + k) % col_count, t, z)) for k in range(col_count)
    ]
    along_col = [
        route(lambda z, t, c, k=k: (z, t, (c + k) % col_count)) for k in range(col_count)
    ]
    along_turn = [route(lambda z, t, c, k=k: (z, (t + k) % ratio, c)) for k in range(ratio)]
    along_plane = [
        route(lambda z, t, c, k=k: ((z + k) % col_count, t, c)) for k in range(col_count)
    ]

    def send(value, pairs):
        return lax.ppermute(value, AXES, pairs)

    def spread_over(values, routes):
        moved = [send(values[k], routes[k]) for k in range(1, len(routes))]
        return [values[0], *moved]

    flagged, *parts = kernel_call(
        functools.partial(flag_body, sizes),
        [((size, n, width), BF16) for size in (freqs, *sizes)],
        [pltpu.VMEM((n * freqs, width), F32)],
        2 * spectra.size,
        (spectra, window_flags),
    )
    side = spread_over([flagged] * col_count, along_col)
    first_sums, second_terms = [], []
    start = 0
    for q, (size, own) in enumerate(zip(sizes, parts)):
        pieces = [send(own, p) for p in to_second]
        (block,) = kernel_call(
            functools.partial(join_body, col_count, ratio),
            [((size, rows, width), BF16)],
            [],
            WAIT_FLOPS,
            pieces,
        )
        second = spread_over([block] * ratio, along_turn)
        last = q == len(sizes) - 1
        sums = [((freqs, n, width), BF16)] * col_count if last else [((size, rows, width), BF16)]
        earlier = first_sums if last else []
        args = (*side, *second, *earlier, pair_mask, misfit_weight, observed)
        outs = kernel_call(
            functools.partial(pair_body, col_count, ratio, start, len(earlier)),
            [((size, rows, width), BF16)] * ratio + sums,
            [
                pltpu.VMEM((size, rows, width), BF16),
                pltpu.VMEM((size, others, width), BF16),
                pltpu.VMEM((size, rows, width), BF16),
                pltpu.VMEM((size, others, width), BF16),
            ],
            12 * size * rows * others * width,
            args,
        )
        halves = spread_over(outs[:ratio], along_turn)
        first_sums += outs[ratio:]
        quarters = kernel_call(
            functools.partial(fold_body, col_count, ratio),
            [((size, n, width), BF16)] * col_count,
            [],
            ratio * halves[0].size,
            halves,
        )
        second_terms += spread_over(quarters, along_plane)
        start += size
    first_terms = spread_over(first_sums[-col_count:], along_col)

    def finish(spans, terms):
        (out,) = kernel_call(
            functools.partial(finish_body, spans),
            [((n, freqs, width), BF16)],
            [pltpu.VMEM((n * freqs, width), F32)],
            col_count * spectra.size,
            terms,
        )
        return out

    grad_first = finish((freqs,), first_terms)
    grad_second = finish(sizes, second_terms)
    return grad_first, grad_second[None]


def solution(mesh):
    placed = (
        P(AXES, None, None),
        P(AXES, None),
        P("row", "col"),
        P(None, "row", "col"),
        P(None, None, "row", "col"),
    )
    row_count, col_count = mesh.shape["row"], mesh.shape["col"]

    def body(*args):
        return per_device(row_count, col_count, *args)

    return jax.shard_map(
        body,
        mesh=mesh,
        in_specs=placed,
        out_specs=(P(AXES, None, None), P("col", "row", None, None)),
        check_vma=False,
    )
```

```python
import functools
import math

import jax
import jax.numpy as jnp
from jax import lax
from jax.experimental import pallas as pl
from jax.experimental.pallas import tpu as pltpu
from jax.sharding import PartitionSpec as P


AXES = ("row", "col")
F32 = jnp.float32
BF16 = jnp.bfloat16
SPARE = 2 << 20
WAIT_FLOPS = 5 * 10**9
UNROLL = 8
CUTS = (0, 8, 16)
PARTS = len(CUTS) - 1
GROUP = 2


def place(ratio):
    row = lax.axis_index("row")
    return row // ratio, row % ratio, lax.axis_index("col")


def spread(col, cols):
    return col // 2 + (col % 2) * (cols // 2)


def unspread(plane, cols):
    return (2 * plane) % cols + (2 * plane) // cols


def at(slot, n):
    return pl.ds(pl.multiple_of(slot * n, n), n)


def kernel_call(body, outs, scratch, flops, args):
    shapes = [jax.ShapeDtypeStruct(*o) for o in outs]
    moved = sum(a.size * a.dtype.itemsize for a in (*args, *shapes))
    held = sum(math.prod(m.shape) * jnp.dtype(m.dtype).itemsize for m in scratch)
    near = pl.BlockSpec(memory_space=pltpu.VMEM)
    return pl.pallas_call(
        body,
        out_shape=shapes,
        in_specs=[near] * len(args),
        out_specs=[near] * len(outs),
        scratch_shapes=scratch,
        compiler_params=pltpu.CompilerParams(vmem_limit_bytes=moved + held + SPARE),
        cost_estimate=pl.CostEstimate(
            flops=flops, bytes_accessed=moved, transcendentals=0
        ),
    )(*args)


def flag_body(spectra, flags, *refs):
    outs, wide = refs[:-1], refs[-1]
    n, freqs, width = spectra.shape
    half = flags.shape[1]
    copies = lax.broadcasted_iota(jnp.int32, (half, width), 1) % half
    copies = (copies == lax.broadcasted_iota(jnp.int32, (half, width), 0)).astype(BF16)
    both = jnp.dot(flags[...].astype(F32).astype(BF16), copies, preferred_element_type=F32)
    wide[...] = spectra[...].astype(F32).reshape(n * freqs, width)
    f = 0
    for out in outs:
        for i in range(out.shape[0]):
            out[i] = (wide[pl.ds(f, n, stride=freqs), :] * both).astype(BF16)
            f += 1


def join_body(ratio, own, mate, out):
    core = place(ratio)[2] % 2
    n = own.shape[1]
    out[:, at(core, n), :] = own[...]
    out[:, at(1 - core, n), :] = mate[...]


def turned(value, width):
    lane = lax.broadcasted_iota(jnp.int32, value.shape, 1)
    sign = jnp.where(lane < width // 2, 1.0, -1.0).astype(F32)
    return pltpu.roll(value.astype(F32), width // 2, 1) * sign


def side_stack(left, f):
    mine = left[f]
    return jnp.concatenate([mine, turned(mine, mine.shape[1]).astype(BF16)], axis=0)


def pair_body(cols, ratio, d, start, *refs):
    half = cols // 2
    side, rest = refs[:half], refs[half:]
    pieces, rest = rest[:half], rest[half:]
    (mask, weight, observed), rest = rest[:3], rest[3:]
    earlier, rest = rest[:d], rest[d:]
    residuals, outs, (left, right, second) = rest[0], rest[1:-3], rest[-3:]
    plane, turn, col = place(ratio)
    freqs, rows, _ = left.shape
    n = rows // cols
    for k in range(half):
        left[:, at((col // 2) ^ k, 2 * n), :] = side[k][...]
        right[:, at(unspread(plane ^ k, cols) // 2, 2 * n), :] = pieces[k][...]
    columns = at(turn ^ d, rows)
    last = d == ratio - 1

    def one(i, _):
        f = start + i
        stack = side_stack(left, i)
        cross = lax.dot_general(
            stack, right[i], (((1,), (1,)), ((), ())), preferred_element_type=F32
        )
        scale = mask[:, columns].astype(F32) * weight[f, :, columns].astype(F32)
        real = scale * (cross[:rows] - observed[0, f, :, columns].astype(F32))
        imag = scale * (cross[rows:] - observed[1, f, :, columns].astype(F32))
        residual = jnp.concatenate([real.astype(BF16), imag.astype(BF16)], axis=0)
        residuals[i] = residual
        sums = lax.dot_general(
            residual, stack, (((0,), (0,)), ((), ())), preferred_element_type=F32
        ).astype(BF16)
        if last:
            second[i, columns] = sums
        else:
            outs[0][i] = sums
        return 0

    lax.fori_loop(0, freqs, one, 0, unroll=min(UNROLL, freqs))
    if not last:
        return
    for e, block in enumerate(earlier):
        second[:, at(turn ^ e, rows), :] = block[...]
    kept, sent = outs[:cols], outs[cols:]
    for m in range(cols):
        slot = (plane ^ m) * ratio
        kept[m][...] = second[:, at(slot + turn, n), :]
        group, spot = divmod(m, GROUP)
        for e in range(1, ratio):
            there = second[:, at(slot + (turn ^ e), n), :]
            sent[group * (ratio - 1) + e - 1][:, spot * n : (spot + 1) * n, :] = there


def first_body(cols, ratio, parts, *refs):
    half = cols // 2
    per = ratio * (half + 1)
    groups, rest = [refs[q * per : (q + 1) * per] for q in range(parts)], refs[parts * per :]
    odd, evens, (right, first) = rest[0], rest[1:-2], rest[-2:]
    plane, _, col = place(ratio)
    _, rows, width = first.shape
    n = rows // cols
    start = 0
    for group in groups:
        pieces, residuals = group[: ratio * half], group[ratio * half :]
        size = residuals[0].shape[0]
        for d in range(ratio):
            for k in range(half):
                slot = d * half + unspread(plane ^ k, cols) // 2
                right[:size, at(slot, 2 * n), :] = pieces[d * half + k][...]

        def one(i, _, residuals=residuals, start=start):
            both = 0.0
            for d in range(ratio):
                other = right[i, d * rows : (d + 1) * rows]
                both += jnp.dot(residuals[d][i], other, preferred_element_type=F32)
            first[start + i] = (both[:rows] - turned(both[rows:], width)).astype(BF16)
            return 0

        lax.fori_loop(0, size, one, 0, unroll=min(UNROLL, size))
        start += size
    for k in range(half):
        evens[k][...] = first[:, at(col ^ (2 * k), n), :]
        odd[:, k * n : (k + 1) * n, :] = first[:, at(col ^ (2 * k + 1), n), :]


def fold_body(spots, *refs):
    terms, out = refs[:-1], refs[-1]
    n = out.shape[1]
    total = 0.0
    for spot, term in zip(spots, terms):
        total += term[:, spot * n : (spot + 1) * n, :].astype(F32)
    out[...] = total.astype(BF16)


def finish_body(spots, parts, *refs):
    out, wide = refs[-2:]
    n, freqs, width = out.shape
    f = 0
    for q in range(parts):
        terms = refs[q * len(spots) : (q + 1) * len(spots)]
        for i in range(terms[0].shape[0]):
            total = 0.0
            for spot, term in zip(spots, terms):
                total += term[i, spot * n : (spot + 1) * n].astype(F32)
            wide[pl.ds(f, n, stride=freqs), :] = total
            f += 1
    out[...] = wide[...].reshape(n, freqs, width).astype(BF16)


def per_device(row_count, cols, spectra, window_flags, pair_mask, misfit_weight, observed):
    ratio = row_count // cols
    half = cols // 2
    n, freqs, width = spectra.shape
    rows = cols * n
    bounds = [freqs * cut // CUTS[-1] for cut in CUTS]
    sizes = [b - a for a, b in zip(bounds, bounds[1:])]

    def send(value, where):
        pairs = []
        for row in range(row_count):
            for col in range(cols):
                plane, turn, to = where(row // ratio, row % ratio, col)
                pairs.append((row * cols + col, (plane * ratio + turn) * cols + to))
        return lax.ppermute(value, AXES, pairs)

    def piece(size, count=1):
        return ((size, count * n, width), BF16)

    owns = kernel_call(
        flag_body,
        [piece(size) for size in sizes],
        [pltpu.VMEM((n * freqs, width), F32)],
        WAIT_FLOPS,
        (spectra, window_flags),
    )
    first_args, second_args = [], []
    for q, (size, own) in enumerate(zip(sizes, owns)):
        mate = send(own, lambda z, t, c: (z, t, c ^ 1))
        (chip,) = kernel_call(
            functools.partial(join_body, ratio), [piece(size, 2)], [], own.size, (own, mate)
        )
        pieces = [send(chip, lambda z, t, c: (spread(c, cols) ^ k, t, z)) for k in range(half)]
        side = [chip] + [send(chip, lambda z, t, c: (z, t, c ^ (2 * k))) for k in range(1, half)]
        for d in range(1, ratio):
            for k in range(half):
                there = send(pieces[k], lambda z, t, c: (z, t ^ d, c))
                pieces.append(there)
        blocks, residuals = [], []
        groups = cols // GROUP
        for d in range(ratio):
            last = d == ratio - 1
            results = [piece(size)] * cols + [piece(size, GROUP)] * (groups * (ratio - 1))
            near = pieces[d * half : (d + 1) * half]
            found, *outs = kernel_call(
                functools.partial(pair_body, cols, ratio, d, bounds[q]),
                [((size, 2 * rows, rows), BF16)] + (results if last else [piece(size, cols)]),
                [
                    pltpu.VMEM((size, rows, width), BF16),
                    pltpu.VMEM((size, rows, width), BF16),
                    pltpu.VMEM((size, rows * ratio, width), BF16),
                ],
                8 * size * rows * rows * width,
                (*side, *near, pair_mask, misfit_weight, observed, *blocks),
            )
            residuals.append(found)
            blocks += outs
        first_args += [*pieces, *residuals]
        kept, sent = blocks[ratio - 1 :][:cols], blocks[ratio - 1 :][cols:]
        back = [[] for _ in range(groups)]
        for g in range(groups):
            for d in range(1, ratio):
                value = sent[g * (ratio - 1) + d - 1]
                there = send(value, lambda z, t, c: (z, t ^ d, c))
                back[g].append(there)
        second_args += [kept[0], *back[0]]
        for m in range(1, cols):
            spots = (0,) + (m % GROUP,) * (ratio - 1)
            (folded,) = kernel_call(
                functools.partial(fold_body, spots),
                [piece(size)],
                [],
                ratio * own.size,
                (kept[m], *back[m // GROUP]),
            )
            there = send(folded, lambda z, t, c: (z ^ m, t, c))
            second_args.append(there)

    odd, *evens = kernel_call(
        functools.partial(first_body, cols, ratio, PARTS),
        [piece(freqs, half)] + [piece(freqs)] * half,
        [
            pltpu.VMEM((max(sizes), rows * ratio, width), BF16),
            pltpu.VMEM((freqs, rows, width), BF16),
        ],
        4 * freqs * rows * rows * ratio * width,
        first_args,
    )
    odd = send(odd, lambda z, t, c: (z, t, c ^ 1))
    first_terms = [evens[0], odd]
    for k in range(1, half):
        (folded,) = kernel_call(
            functools.partial(fold_body, (0, k)), [piece(freqs)], [], n, (evens[k], odd)
        )
        there = send(folded, lambda z, t, c: (z, t, c ^ (2 * k)))
        first_terms.append(there)

    def finish(parts, terms):
        (out,) = kernel_call(
            functools.partial(finish_body, (0,) * (len(terms) // parts), parts),
            [((n, freqs, width), BF16)],
            [pltpu.VMEM((n * freqs, width), F32)],
            cols * spectra.size,
            terms,
        )
        return out

    grad_first = finish(1, first_terms)
    return grad_first, finish(PARTS, second_args)[None]


def solution(mesh):
    placed = (
        P(AXES, None, None),
        P(AXES, None),
        P("row", "col"),
        P(None, "row", "col"),
        P(None, None, "row", "col"),
    )
    row_count, cols = mesh.shape["row"], mesh.shape["col"]
    ratio = row_count // cols
    for count in (cols, ratio):
        assert count & (count - 1) == 0 and cols % GROUP == 0 and cols > 1, "mesh sizes"

    def body(*args):
        return per_device(row_count, cols, *args)

    return jax.shard_map(
        body,
        mesh=mesh,
        in_specs=placed,
        out_specs=(P(AXES, None, None), P("col", "row", None, None)),
        check_vma=False,
    )
```

```python
import functools
import math

import jax
import jax.numpy as jnp
from jax import lax
from jax.experimental import pallas as pl
from jax.experimental.pallas import tpu as pltpu
from jax.sharding import PartitionSpec as P


AXES = ("row", "col")
F32 = jnp.float32
BF16 = jnp.bfloat16
SPARE = 2 << 20
WAIT_FLOPS = 5 * 10**9
UNROLL = 8
CUTS = (0, 8, 16)
PARTS = len(CUTS) - 1
GROUP = 2


def place(ratio):
    row = lax.axis_index("row")
    return row // ratio, row % ratio, lax.axis_index("col")


def spread(col, cols):
    return col // 2 + (col % 2) * (cols // 2)


def unspread(plane, cols):
    return (2 * plane) % cols + (2 * plane) // cols


def at(slot, n):
    return pl.ds(pl.multiple_of(slot * n, n), n)


def kernel_call(body, outs, scratch, flops, args):
    shapes = [jax.ShapeDtypeStruct(*o) for o in outs]
    moved = sum(a.size * a.dtype.itemsize for a in (*args, *shapes))
    held = sum(math.prod(m.shape) * jnp.dtype(m.dtype).itemsize for m in scratch)
    near = pl.BlockSpec(memory_space=pltpu.VMEM)
    return pl.pallas_call(
        body,
        out_shape=shapes,
        in_specs=[near] * len(args),
        out_specs=[near] * len(outs),
        scratch_shapes=scratch,
        compiler_params=pltpu.CompilerParams(vmem_limit_bytes=moved + held + SPARE),
        cost_estimate=pl.CostEstimate(
            flops=flops, bytes_accessed=moved, transcendentals=0
        ),
    )(*args)


def bits_body(flags, out):
    half, width = flags.shape[1], out.shape[1]
    copies = lax.broadcasted_iota(jnp.int32, (half, width), 1) % half
    copies = (copies == lax.broadcasted_iota(jnp.int32, (half, width), 0)).astype(BF16)
    out[...] = jnp.dot(flags[...].astype(F32).astype(BF16), copies, preferred_element_type=F32)


def flag_body(spectra, both, out, wide):
    n, freqs, width = spectra.shape
    wide[...] = spectra[...].astype(F32).reshape(n * freqs, width)
    for f in range(freqs):
        out[f] = (wide[pl.ds(f, n, stride=freqs), :] * both[...]).astype(BF16)


def join_body(ratio, bounds, own, mate, *outs):
    core = place(ratio)[2] % 2
    n = own.shape[1]
    whole = outs[0]
    whole[:, at(core, n), :] = own[...]
    whole[:, at(1 - core, n), :] = mate[...]
    for q, out in enumerate(outs[1:]):
        part = slice(bounds[q], bounds[q + 1])
        out[:, at(core, n), :] = own[part]
        out[:, at(1 - core, n), :] = mate[part]


def stack_body(*refs):
    pieces, out = refs[:-1], refs[-1]
    n = pieces[0].shape[1]
    for k, value in enumerate(pieces):
        out[:, k * n : (k + 1) * n, :] = value[...]


def unroll_of(steps):
    return max(u for u in range(1, UNROLL + 1) if steps % u == 0)


def turned(value, width):
    lane = lax.broadcasted_iota(jnp.int32, value.shape, 1)
    sign = jnp.where(lane < width // 2, 1.0, -1.0).astype(F32)
    return pltpu.roll(value.astype(F32), width // 2, 1) * sign


def side_stack(left, f):
    mine = left[f]
    return jnp.concatenate([mine, turned(mine, mine.shape[1]).astype(BF16)], axis=0)


def taken(pieces, k, n):
    return pieces[k][...] if len(pieces) > 1 else pieces[0][:, k * n : (k + 1) * n, :]


def pair_body(cols, ratio, d, start, *refs):
    half = cols // 2
    side, rest = refs[:half], refs[half:]
    pieces, rest = (rest[:1], rest[1:]) if d else (rest[:half], rest[half:])
    (mask, weight, observed), rest = rest[:3], rest[3:]
    earlier, rest = rest[:d], rest[d:]
    residuals, outs, (left, right, second) = rest[0], rest[1:-3], rest[-3:]
    plane, turn, col = place(ratio)
    freqs, rows, _ = left.shape
    n = rows // cols
    for k in range(half):
        left[:, at((col // 2) ^ k, 2 * n), :] = side[k][start : start + freqs]
        right[:, at(unspread(plane ^ k, cols) // 2, 2 * n), :] = taken(pieces, k, 2 * n)
    columns = at(turn ^ d, rows)
    last = d == ratio - 1

    def one(i, _):
        f = start + i
        stack = side_stack(left, i)
        cross = lax.dot_general(
            stack, right[i], (((1,), (1,)), ((), ())), preferred_element_type=F32
        )
        scale = mask[:, columns].astype(F32) * weight[f, :, columns].astype(F32)
        real = scale * (cross[:rows] - observed[0, f, :, columns].astype(F32))
        imag = scale * (cross[rows:] - observed[1, f, :, columns].astype(F32))
        residual = jnp.concatenate([real.astype(BF16), imag.astype(BF16)], axis=0)
        residuals[i] = residual
        sums = lax.dot_general(
            residual, stack, (((0,), (0,)), ((), ())), preferred_element_type=F32
        ).astype(BF16)
        if last:
            second[i, columns] = sums
        else:
            outs[0][i] = sums
        return 0

    lax.fori_loop(0, freqs, one, 0, unroll=unroll_of(freqs))
    if not last:
        return
    for e, block in enumerate(earlier):
        second[:, at(turn ^ e, rows), :] = block[...]
    kept, sent = outs[:cols], outs[cols:]
    for m in range(cols):
        slot = (plane ^ m) * ratio
        kept[m][...] = second[:, at(slot + turn, n), :]
        group, spot = divmod(m, GROUP)
        for e in range(1, ratio):
            there = second[:, at(slot + (turn ^ e), n), :]
            sent[group * (ratio - 1) + e - 1][:, spot * n : (spot + 1) * n, :] = there


def first_body(cols, ratio, parts, *refs):
    half = cols // 2
    per = half + 2 * ratio - 1
    groups, rest = [refs[q * per : (q + 1) * per] for q in range(parts)], refs[parts * per :]
    odd, evens, (right, first) = rest[0], rest[1:-2], rest[-2:]
    plane, _, col = place(ratio)
    _, rows, width = first.shape
    n = rows // cols
    start = 0
    for group in groups:
        pieces, residuals = group[: half + ratio - 1], group[half + ratio - 1 :]
        pieces = [pieces[:half], *([p] for p in pieces[half:])]
        size = residuals[0].shape[0]
        for d in range(ratio):
            for k in range(half):
                slot = d * half + unspread(plane ^ k, cols) // 2
                right[:size, at(slot, 2 * n), :] = taken(pieces[d], k, 2 * n)

        def one(i, _, residuals=residuals, start=start):
            both = 0.0
            for d in range(ratio):
                other = right[i, d * rows : (d + 1) * rows]
                both += jnp.dot(residuals[d][i], other, preferred_element_type=F32)
            first[start + i] = (both[:rows] - turned(both[rows:], width)).astype(BF16)
            return 0

        lax.fori_loop(0, size, one, 0, unroll=unroll_of(size))
        start += size
    for k in range(half):
        evens[k][...] = first[:, at(col ^ (2 * k), n), :]
        odd[:, k * n : (k + 1) * n, :] = first[:, at(col ^ (2 * k + 1), n), :]


def fold_body(spots, *refs):
    terms, out = refs[:-1], refs[-1]
    n = out.shape[1]
    total = 0.0
    for spot, term in zip(spots, terms):
        total += term[:, spot * n : (spot + 1) * n, :].astype(F32)
    out[...] = total.astype(BF16)


def finish_body(count, parts, *refs):
    outs, wide = refs[-3:-1], refs[-1]
    n, freqs, width = outs[0].shape
    groups = [refs[:count]] + [refs[count + q : -3 : parts] for q in range(parts)]
    for out, sets in ((outs[0], groups[:1]), (outs[1], groups[1:])):
        f = 0
        for terms in sets:
            for i in range(terms[0].shape[0]):
                total = 0.0
                for term in terms:
                    total += term[i, :n].astype(F32)
                wide[pl.ds(f, n, stride=freqs), :] = total
                f += 1
        out[...] = wide[...].reshape(n, freqs, width).astype(BF16)


def per_device(row_count, cols, spectra, window_flags, pair_mask, misfit_weight, observed):
    ratio = row_count // cols
    half = cols // 2
    n, freqs, width = spectra.shape
    rows = cols * n
    bounds = [freqs * cut // CUTS[-1] for cut in CUTS]
    sizes = [b - a for a, b in zip(bounds, bounds[1:])]

    def send(value, where):
        pairs = []
        for row in range(row_count):
            for col in range(cols):
                plane, turn, to = where(row // ratio, row % ratio, col)
                pairs.append((row * cols + col, (plane * ratio + turn) * cols + to))
        return lax.ppermute(value, AXES, pairs)

    def piece(size, count=1):
        return ((size, count * n, width), BF16)

    (both,) = kernel_call(
        bits_body, [((n, width), F32)], [], WAIT_FLOPS, (window_flags,)
    )
    (own,) = kernel_call(
        flag_body,
        [piece(freqs)],
        [pltpu.VMEM((n * freqs, width), F32)],
        WAIT_FLOPS,
        (spectra, both),
    )
    mate = send(own, lambda z, t, c: (z, t, c ^ 1))
    chip, *chips = kernel_call(
        functools.partial(join_body, ratio, bounds),
        [piece(freqs, 2)] + [piece(size, 2) for size in sizes],
        [],
        own.size,
        (own, mate),
    )
    side = [chip] + [
        send(chip, lambda z, t, c: (z, t, c ^ (2 * k))) for k in range(1, half)
    ]
    first_args, second_args = [], []
    for q, size in enumerate(sizes):
        pieces = [
            send(chips[q], lambda z, t, c: (spread(c, cols) ^ k, t, z))
            for k in range(half)
        ]
        (stack,) = kernel_call(stack_body, [piece(size, cols)], [], own.size, pieces)
        for d in range(1, ratio):
            pieces.append(send(stack, lambda z, t, c: (z, t ^ d, c)))
        blocks, residuals = [], []
        groups = cols // GROUP
        for d in range(ratio):
            last = d == ratio - 1
            results = [piece(size)] * cols + [piece(size, GROUP)] * (groups * (ratio - 1))
            near = pieces[half + d - 1 : half + d] if d else pieces[:half]
            found, *outs = kernel_call(
                functools.partial(pair_body, cols, ratio, d, bounds[q]),
                [((size, 2 * rows, rows), BF16)] + (results if last else [piece(size, cols)]),
                [
                    pltpu.VMEM((size, rows, width), BF16),
                    pltpu.VMEM((size, rows, width), BF16),
                    pltpu.VMEM((size, rows * ratio, width), BF16),
                ],
                8 * size * rows * rows * width,
                (*side, *near, pair_mask, misfit_weight, observed, *blocks),
            )
            residuals.append(found)
            blocks += outs
        first_args += [*pieces, *residuals]
        kept, sent = blocks[ratio - 1 :][:cols], blocks[ratio - 1 :][cols:]
        back = [[] for _ in range(groups)]
        for g in range(groups):
            for d in range(1, ratio):
                value = sent[g * (ratio - 1) + d - 1]
                there = send(value, lambda z, t, c: (z, t ^ d, c))
                back[g].append(there)
        second_args.append([kept[0], *back[0]])
        for m in range(1, cols):
            spots = (0,) + (m % GROUP,) * (ratio - 1)
            (folded,) = kernel_call(
                functools.partial(fold_body, spots),
                [piece(size)],
                [],
                size * n,
                (kept[m], *back[m // GROUP]),
            )
            there = send(folded, lambda z, t, c: (z ^ m, t, c))
            second_args[q].append(there)

    odd, *evens = kernel_call(
        functools.partial(first_body, cols, ratio, PARTS),
        [piece(freqs, half)] + [piece(freqs)] * half,
        [
            pltpu.VMEM((max(sizes), rows * ratio, width), BF16),
            pltpu.VMEM((freqs, rows, width), BF16),
        ],
        4 * freqs * rows * rows * ratio * width,
        first_args,
    )
    odd = send(odd, lambda z, t, c: (z, t, c ^ 1))
    first_terms = [evens[0], odd]
    for k in range(1, half):
        (folded,) = kernel_call(
            functools.partial(fold_body, (0, k)), [piece(freqs)], [], n, (evens[k], odd)
        )
        there = send(folded, lambda z, t, c: (z, t, c ^ (2 * k)))
        first_terms.append(there)

    grad_first, grad_second = kernel_call(
        functools.partial(finish_body, len(first_terms), PARTS),
        [((n, freqs, width), BF16)] * 2,
        [pltpu.VMEM((n * freqs, width), F32)],
        cols * spectra.size,
        first_terms + [term for terms in zip(*second_args) for term in terms],
    )
    return grad_first, grad_second[None]


def solution(mesh):
    placed = (
        P(AXES, None, None),
        P(AXES, None),
        P("row", "col"),
        P(None, "row", "col"),
        P(None, None, "row", "col"),
    )
    row_count, cols = mesh.shape["row"], mesh.shape["col"]
    ratio = row_count // cols
    for count in (cols, ratio):
        assert count & (count - 1) == 0 and cols % GROUP == 0 and cols > 1, "mesh sizes"

    def body(*args):
        return per_device(row_count, cols, *args)

    return jax.shard_map(
        body,
        mesh=mesh,
        in_specs=placed,
        out_specs=(P(AXES, None, None), P("col", "row", None, None)),
        check_vma=False,
    )
```

```python
import functools
import math

import jax
import jax.numpy as jnp
from jax import lax
from jax.experimental import pallas as pl
from jax.experimental.pallas import tpu as pltpu
from jax.sharding import PartitionSpec as P


AXES = ("row", "col")
F32 = jnp.float32
BF16 = jnp.bfloat16
SPARE = 2 << 20
WAIT_FLOPS = 5 * 10**9
UNROLL = 8
CUTS = (0, 8, 16)
PARTS = len(CUTS) - 1
GROUP = 2


def place(ratio):
    row = lax.axis_index("row")
    return row // ratio, row % ratio, lax.axis_index("col")


def spread(col, cols):
    return col // 2 + (col % 2) * (cols // 2)


def unspread(plane, cols):
    return (2 * plane) % cols + (2 * plane) // cols


def at(slot, n):
    return pl.ds(pl.multiple_of(slot * n, n), n)


def kernel_call(body, outs, scratch, flops, args, place_out=pltpu.VMEM):
    shapes = [jax.ShapeDtypeStruct(*o) for o in outs]
    moved = sum(a.size * a.dtype.itemsize for a in (*args, *shapes))
    held = sum(
        math.prod(m.shape) * jnp.dtype(m.dtype).itemsize
        for m in scratch
        if m.memory_space == pltpu.VMEM
    )
    near = pl.BlockSpec(memory_space=pltpu.VMEM)
    return pl.pallas_call(
        body,
        out_shape=shapes,
        in_specs=[near] * len(args),
        out_specs=[pl.BlockSpec(memory_space=place_out)] * len(outs),
        scratch_shapes=scratch,
        compiler_params=pltpu.CompilerParams(vmem_limit_bytes=moved + held + SPARE),
        cost_estimate=pl.CostEstimate(
            flops=flops, bytes_accessed=moved, transcendentals=0
        ),
    )(*args)


def bits_body(flags, out):
    half, width = flags.shape[1], out.shape[1]
    copies = lax.broadcasted_iota(jnp.int32, (half, width), 1) % half
    copies = (copies == lax.broadcasted_iota(jnp.int32, (half, width), 0)).astype(BF16)
    out[...] = jnp.dot(flags[...].astype(F32).astype(BF16), copies, preferred_element_type=F32)


def flag_body(spectra, both, out, wide):
    n, freqs, width = spectra.shape
    wide[...] = spectra[...].astype(F32).reshape(n * freqs, width)
    for f in range(freqs):
        out[f] = (wide[pl.ds(f, n, stride=freqs), :] * both[...]).astype(BF16)


def join_body(ratio, bounds, own, mate, *outs):
    core = place(ratio)[2] % 2
    n = own.shape[1]
    whole = outs[0]
    whole[:, at(core, n), :] = own[...]
    whole[:, at(1 - core, n), :] = mate[...]
    for q, out in enumerate(outs[1:]):
        part = slice(bounds[q], bounds[q + 1])
        out[:, at(core, n), :] = own[part]
        out[:, at(1 - core, n), :] = mate[part]


def stack_body(*refs):
    pieces, out = refs[:-1], refs[-1]
    n = pieces[0].shape[1]
    for k, value in enumerate(pieces):
        out[:, k * n : (k + 1) * n, :] = value[...]


def unroll_of(steps):
    return max(u for u in range(1, UNROLL + 1) if steps % u == 0)


def turned(value, width):
    lane = lax.broadcasted_iota(jnp.int32, value.shape, 1)
    sign = jnp.where(lane < width // 2, 1.0, -1.0).astype(F32)
    return pltpu.roll(value.astype(F32), width // 2, 1) * sign


def side_stack(left, f):
    mine = left[f]
    return jnp.concatenate([mine, turned(mine, mine.shape[1]).astype(BF16)], axis=0)


def taken(pieces, k, n):
    return pieces[k][...] if len(pieces) > 1 else pieces[0][:, k * n : (k + 1) * n, :]


def pair_body(cols, ratio, d, start, *refs):
    half = cols // 2
    side, rest = refs[:half], refs[half:]
    pieces, rest = (rest[:1], rest[1:]) if d else (rest[:half], rest[half:])
    (mask, weight, observed), rest = rest[:3], rest[3:]
    earlier, rest = rest[:d], rest[d:]
    residuals, outs, (left, right, second) = rest[0], rest[1:-3], rest[-3:]
    plane, turn, col = place(ratio)
    freqs, rows, _ = left.shape
    n = rows // cols
    for k in range(half):
        left[:, at((col // 2) ^ k, 2 * n), :] = side[k][start : start + freqs]
        right[:, at(unspread(plane ^ k, cols) // 2, 2 * n), :] = taken(pieces, k, 2 * n)
    columns = at(turn ^ d, rows)
    last = d == ratio - 1

    def one(i, _):
        f = start + i
        stack = side_stack(left, i)
        cross = lax.dot_general(
            stack, right[i], (((1,), (1,)), ((), ())), preferred_element_type=F32
        )
        scale = mask[:, columns].astype(F32) * weight[f, :, columns].astype(F32)
        real = scale * (cross[:rows] - observed[0, f, :, columns].astype(F32))
        imag = scale * (cross[rows:] - observed[1, f, :, columns].astype(F32))
        residual = jnp.concatenate([real.astype(BF16), imag.astype(BF16)], axis=0)
        residuals[i] = residual
        sums = lax.dot_general(
            residual, stack, (((0,), (0,)), ((), ())), preferred_element_type=F32
        ).astype(BF16)
        if last:
            second[i, columns] = sums
        else:
            outs[0][i] = sums
        return 0

    lax.fori_loop(0, freqs, one, 0, unroll=unroll_of(freqs))
    if not last:
        return
    for e, block in enumerate(earlier):
        second[:, at(turn ^ e, rows), :] = block[...]
    kept, sent = outs[:cols], outs[cols:]
    for m in range(cols):
        slot = (plane ^ m) * ratio
        kept[m][...] = second[:, at(slot + turn, n), :]
        group, spot = divmod(m, GROUP)
        for e in range(1, ratio):
            there = second[:, at(slot + (turn ^ e), n), :]
            sent[group * (ratio - 1) + e - 1][:, spot * n : (spot + 1) * n, :] = there


def first_body(cols, ratio, parts, *refs):
    half = cols // 2
    per = half + 2 * ratio - 1
    groups, rest = [refs[q * per : (q + 1) * per] for q in range(parts)], refs[parts * per :]
    odd, evens, (right, first) = rest[0], rest[1:-2], rest[-2:]
    plane, _, col = place(ratio)
    _, rows, width = first.shape
    n = rows // cols
    start = 0
    for group in groups:
        pieces, residuals = group[: half + ratio - 1], group[half + ratio - 1 :]
        pieces = [pieces[:half], *([p] for p in pieces[half:])]
        size = residuals[0].shape[0]
        for d in range(ratio):
            for k in range(half):
                slot = d * half + unspread(plane ^ k, cols) // 2
                right[:size, at(slot, 2 * n), :] = taken(pieces[d], k, 2 * n)

        def one(i, _, residuals=residuals, start=start):
            both = 0.0
            for d in range(ratio):
                other = right[i, d * rows : (d + 1) * rows]
                both += jnp.dot(residuals[d][i], other, preferred_element_type=F32)
            first[start + i] = (both[:rows] - turned(both[rows:], width)).astype(BF16)
            return 0

        lax.fori_loop(0, size, one, 0, unroll=unroll_of(size))
        start += size
    for k in range(half):
        evens[k][...] = first[:, at(col ^ (2 * k), n), :]
        odd[:, k * n : (k + 1) * n, :] = first[:, at(col ^ (2 * k + 1), n), :]


def fold_body(spots, *refs):
    terms, out = refs[:-1], refs[-1]
    n = out.shape[1]
    total = 0.0
    for spot, term in zip(spots, terms):
        total += term[:, spot * n : (spot + 1) * n, :].astype(F32)
    out[...] = total.astype(BF16)


def finish_body(count, parts, *refs):
    outs, (wide, staged, sems) = refs[-5:-3], refs[-3:]
    n, freqs, width = outs[0].shape
    copies = []
    groups = [refs[:count]] + [refs[count + q : -5 : parts] for q in range(parts)]
    for which, sets in enumerate((groups[:1], groups[1:])):
        f = 0
        for terms in sets:
            for i in range(terms[0].shape[0]):
                total = 0.0
                for term in terms:
                    total += term[i, :n].astype(F32)
                wide[which, pl.ds(f, n, stride=freqs), :] = total
                f += 1
        staged[which] = wide[which].reshape(n, freqs, width).astype(BF16)
        copies.append(pltpu.make_async_copy(staged.at[which], outs[which], sems.at[which]))
        copies[-1].start()
    for copy in copies:
        copy.wait()


def per_device(row_count, cols, spectra, window_flags, pair_mask, misfit_weight, observed):
    ratio = row_count // cols
    half = cols // 2
    n, freqs, width = spectra.shape
    rows = cols * n
    bounds = [freqs * cut // CUTS[-1] for cut in CUTS]
    sizes = [b - a for a, b in zip(bounds, bounds[1:])]

    def send(value, where):
        pairs = []
        for row in range(row_count):
            for col in range(cols):
                plane, turn, to = where(row // ratio, row % ratio, col)
                pairs.append((row * cols + col, (plane * ratio + turn) * cols + to))
        return lax.ppermute(value, AXES, pairs)

    def piece(size, count=1):
        return ((size, count * n, width), BF16)

    (both,) = kernel_call(bits_body, [((n, width), F32)], [], WAIT_FLOPS, (window_flags,))
    (own,) = kernel_call(
        flag_body,
        [piece(freqs)],
        [pltpu.VMEM((n * freqs, width), F32)],
        WAIT_FLOPS,
        (spectra, both),
    )
    mate = send(own, lambda z, t, c: (z, t, c ^ 1))
    chip, *chips = kernel_call(
        functools.partial(join_body, ratio, bounds),
        [piece(freqs, 2)] + [piece(size, 2) for size in sizes],
        [],
        own.size,
        (own, mate),
    )
    side = [chip] + [send(chip, lambda z, t, c: (z, t, c ^ (2 * k))) for k in range(1, half)]
    first_args, second_args = [], []
    for q, size in enumerate(sizes):
        pieces = [send(chips[q], lambda z, t, c: (spread(c, cols) ^ k, t, z)) for k in range(half)]
        (stack,) = kernel_call(stack_body, [piece(size, cols)], [], own.size, pieces)
        for d in range(1, ratio):
            pieces.append(send(stack, lambda z, t, c: (z, t ^ d, c)))
        blocks, residuals = [], []
        groups = cols // GROUP
        for d in range(ratio):
            last = d == ratio - 1
            results = [piece(size)] * cols + [piece(size, GROUP)] * (groups * (ratio - 1))
            near = pieces[half + d - 1 : half + d] if d else pieces[:half]
            found, *outs = kernel_call(
                functools.partial(pair_body, cols, ratio, d, bounds[q]),
                [((size, 2 * rows, rows), BF16)] + (results if last else [piece(size, cols)]),
                [
                    pltpu.VMEM((size, rows, width), BF16),
                    pltpu.VMEM((size, rows, width), BF16),
                    pltpu.VMEM((size, rows * ratio, width), BF16),
                ],
                8 * size * rows * rows * width,
                (*side, *near, pair_mask, misfit_weight, observed, *blocks),
            )
            residuals.append(found)
            blocks += outs
        first_args += [*pieces, *residuals]
        kept, sent = blocks[ratio - 1 :][:cols], blocks[ratio - 1 :][cols:]
        back = [[] for _ in range(groups)]
        for g in range(groups):
            for d in range(1, ratio):
                value = sent[g * (ratio - 1) + d - 1]
                there = send(value, lambda z, t, c: (z, t ^ d, c))
                back[g].append(there)
        second_args.append([kept[0], *back[0]])
        for m in range(1, cols):
            spots = (0,) + (m % GROUP,) * (ratio - 1)
            (folded,) = kernel_call(
                functools.partial(fold_body, spots),
                [piece(size)],
                [],
                size * n,
                (kept[m], *back[m // GROUP]),
            )
            there = send(folded, lambda z, t, c: (z ^ m, t, c))
            second_args[q].append(there)

    odd, *evens = kernel_call(
        functools.partial(first_body, cols, ratio, PARTS),
        [piece(freqs, half)] + [piece(freqs)] * half,
        [
            pltpu.VMEM((max(sizes), rows * ratio, width), BF16),
            pltpu.VMEM((freqs, rows, width), BF16),
        ],
        4 * freqs * rows * rows * ratio * width,
        first_args,
    )
    odd = send(odd, lambda z, t, c: (z, t, c ^ 1))
    first_terms = [evens[0], odd]
    for k in range(1, half):
        (folded,) = kernel_call(
            functools.partial(fold_body, (0, k)), [piece(freqs)], [], n, (evens[k], odd)
        )
        there = send(folded, lambda z, t, c: (z, t, c ^ (2 * k)))
        first_terms.append(there)

    grad_first, grad_second = kernel_call(
        functools.partial(finish_body, len(first_terms), PARTS),
        [((n, freqs, width), BF16)] * 2,
        [
            pltpu.VMEM((2, n * freqs, width), F32),
            pltpu.VMEM((2, n, freqs, width), BF16),
            pltpu.SemaphoreType.DMA((2,)),
        ],
        cols * spectra.size,
        first_terms + [term for terms in zip(*second_args) for term in terms],
        pltpu.HBM,
    )
    return grad_first, grad_second[None]


def solution(mesh):
    placed = (
        P(AXES, None, None),
        P(AXES, None),
        P("row", "col"),
        P(None, "row", "col"),
        P(None, None, "row", "col"),
    )
    row_count, cols = mesh.shape["row"], mesh.shape["col"]
    ratio = row_count // cols
    for count in (cols, ratio):
        assert count & (count - 1) == 0 and cols % GROUP == 0 and cols > 1, "mesh sizes"

    def body(*args):
        return per_device(row_count, cols, *args)

    return jax.shard_map(
        body,
        mesh=mesh,
        in_specs=placed,
        out_specs=(P(AXES, None, None), P("col", "row", None, None)),
        check_vma=False,
    )
```
